32 devices in a mesh: grp: 2 (over y), dp: 4 (over z), tp: 4 (over x, core).
Axes of the slice: x: 2, y: 2, z: 4, core: 2. Of those that a mesh axis runs over, the one named last changes fastest.
Arguments:
- tiers: bfloat16 [512, 24576], P('dp', ('grp', 'tp')), may hold values from -6 to 6
- w_merge: bfloat16 [24576, 8192], P(('grp', 'tp'), 'dp'), may hold values from -0.0390625 to 0.0390625
- norm_gain: float32 [8192], P('dp'), may hold values from 0.4 to 1.6
- w_head: bfloat16 [8192, 32000], P('dp', ('grp', 'tp')), may hold values from -0.1875 to 0.1875
- token_ids: int32 [512], P('dp'), may hold values from 0 to 31999
- labels: int32 [512], P('dp'), may hold values from 0 to 7
- quotas: int32 [8], replicated, may hold values from 16 to 47
Outputs:
- normed: bfloat16 [512, 8192], P(('grp', 'tp'), 'dp')
- row_loss: float32 [512], P('dp')
The draws below stay inside these ranges and needn't reach their ends.
All inputs are finite; a program needn't handle non-finite values.
Results may differ from the reference program's by a relative error of at most 0.008.
Values may be sent and summed in bfloat16 or wider, within the bound.
No kernel may reach another device: no remote copies, remote signals or barrier semaphores. Data moves between devices by JAX's collectives and lax.ppermute only.
A program may use at most 64 MiB of HBM per device.

```python
import math
import jax
import jax.numpy as jnp
import numpy as np
from jax import lax

D = 8192
V = 32000
DOMAINS = 8
TOKENS = 512


def with_ends(values, stream_key, smallest, largest):
    place = [jax.random.randint(jax.random.fold_in(stream_key, axis), (), 0, length) for axis, length in enumerate(values.shape)]
    longest = values.shape.index(max(values.shape))
    neighbour = place[:longest] + [(place[longest] + 1) % values.shape[longest]] + place[longest + 1:]
    return values.at[tuple(place)].set(smallest).at[tuple(neighbour)].set(largest)


def block_levels(stream_key, extent, pieces, smallest, largest):
    loudness = 1.0
    for dim, shards_of in pieces:
        steps = jax.random.uniform(jax.random.fold_in(jax.random.fold_in(stream_key, 6), dim), (shards_of,), jnp.float32, smallest / len(pieces), largest / len(pieces))
        loudness = loudness * jnp.repeat(jnp.exp(steps), extent[dim] // shards_of).reshape((-1,) + (1,) * (len(extent) - 1 - dim))
    return loudness


def rank_bounds(number_of, skew):
    portions = [(1 << 20) // math.isqrt(standing ** skew) + 1 for standing in range(1, number_of + 1)]
    width = 1 + sum(portions) // (1 << 30)
    return np.cumsum(np.array([max(1, weight // width) for weight in portions]))


def ranked(own_key, shape, count, slope):
    table = rank_bounds(count, slope)
    ticket = jax.random.randint(jax.random.fold_in(own_key, 1), shape, 0, int(table[count - 1]))
    standing = jnp.searchsorted(jnp.asarray(table, jnp.int32), ticket, side="right")
    return jax.random.permutation(jax.random.fold_in(own_key, 2), count)[standing].astype(jnp.int32)


def bell_draw(key, extent, spread, reach, shards=(), kind=jnp.bfloat16):
    values = spread * jax.random.normal(key, extent, jnp.float32)
    if shards:
        values = values * block_levels(key, extent, shards, -0.22, 0.18)
    return jnp.clip(values, -reach, reach).astype(kind)


def setup_inputs(seed: int = 0) -> dict:
    keys = jax.random.split(jax.random.key(seed), 8)
    tiers = bell_draw(keys[0], (TOKENS, 3 * D), 1.0, 6.0, ((0, 4), (1, 8)))
    w_merge = bell_draw(keys[1], (3 * D, D), (3 * D) ** -0.5, 0.0390625, ((0, 8), (1, 4)))
    norm_gain = jnp.clip(1.0 + 0.12 * jax.random.normal(keys[2], (D,), jnp.float32), 0.4, 1.6)
    w_head = bell_draw(keys[3], (D, V), (D // 9) ** -0.5, 0.1875, ((0, 4), (1, 8)))
    token_ids = with_ends(ranked(keys[4], (TOKENS,), V, 2), jax.random.fold_in(keys[4], 3), 0, V - 1).astype(jnp.int32)
    labels = with_ends(jax.random.randint(keys[5], (TOKENS,), 0, DOMAINS), jax.random.fold_in(keys[5], 1), 0, DOMAINS - 1).astype(jnp.int32)
    quotas = with_ends(jax.random.randint(keys[6], (DOMAINS,), TOKENS // (4 * DOMAINS), 3 * TOKENS // (4 * DOMAINS)), jax.random.fold_in(keys[6], 1), TOKENS // (4 * DOMAINS), (3 * TOKENS // (4 * DOMAINS)) - 1).astype(jnp.int32)
    return {"tiers": tiers, "w_merge": w_merge, "norm_gain": norm_gain, "w_head": w_head, "token_ids": token_ids, "labels": labels, "quotas": quotas}


def reference(tiers, w_merge, norm_gain, w_head, token_ids, labels, quotas):
    merged = jnp.dot(tiers, w_merge, preferred_element_type=jnp.float32)
    squares = lax.optimization_barrier(jnp.mean(merged * merged, axis=1))
    normed = (merged * lax.rsqrt(squares + 1e-05)[:, None] * norm_gain[None, :]).astype(jnp.bfloat16)
    logits = jnp.dot(normed, w_head, preferred_element_type=jnp.float32)
    sumexp = lax.optimization_barrier(jnp.sum(jnp.exp(logits), axis=1))
    target = jnp.take_along_axis(logits, token_ids.astype(jnp.int32)[:, None], axis=1)[:, 0]
    loss = jnp.log(sumexp) - target
    onehot = (labels[:, None] == jnp.arange(DOMAINS, dtype=jnp.int32)[None, :]).astype(jnp.int32)
    earlier = jnp.cumsum(onehot, axis=0) - onehot
    rank = lax.optimization_barrier(jnp.sum(earlier * onehot, axis=1))
    allowed = lax.optimization_barrier(jnp.sum(onehot * quotas[None, :], axis=1))
    row_loss = jnp.where(rank < allowed, loss, jnp.float32(0.0))
    return (normed, row_loss)
```

```python
import jax
import jax.numpy as jnp
from jax import lax
from jax.sharding import PartitionSpec as P

DOMAINS = 8
CORES = 2
EPS = 1e-05
BF16, F32, I32 = jnp.bfloat16, jnp.float32, jnp.int32
PLANE = ("grp", "tp")


def pick(blocks, index):
    return lax.dynamic_index_in_dim(blocks, index, 0, keepdims=False)


def on_device(sizes, tiers, w_merge, norm_gain, w_head, token_ids, labels, quotas):
    groups, depth, across = sizes
    chips = groups * across // CORES
    z = lax.axis_index("dp")
    member = lax.axis_index(PLANE)
    core, chip = member % CORES, member // CORES
    chunk, width = tiers.shape[0], w_merge.shape[1]
    rows = chunk * depth
    vocab = w_head.shape[1]
    cap = rows * 3 // 4
    owned = -(-vocab // depth // 8) * 8

    def to_chip(value, k):
        pairs = [(m, (((m // CORES) ^ k) * CORES) + m % CORES) for m in range(groups * across)]
        return lax.ppermute(value, PLANE, pairs)

    def to_core(value):
        return lax.ppermute(value, PLANE, [(m, m ^ 1) for m in range(groups * across)])

    def around(value):
        got = [value]
        for k in range(1, depth):
            got.append(lax.ppermute(value, "dp", [(i, (i + k) % depth) for i in range(depth)]))
        got = jnp.stack(got)
        return jnp.stack([pick(got, (z - k) % depth) for k in range(depth)])

    def merge(x):
        return jnp.dot(x, w_merge, preferred_element_type=F32)

    def core_sum(part):
        n = part.shape[0] // CORES
        part = part.reshape(CORES, n, width)
        other = to_core(pick(part, 1 - core).astype(BF16))
        return pick(part, core) + other.astype(F32)

    def both_cores(mine):
        other = to_core(mine)
        first = core == 0
        return jnp.concatenate([jnp.where(first, mine, other), jnp.where(first, other, mine)])

    def sum_direct(part):
        mine = core_sum(part).astype(BF16)
        got = [mine] + [to_chip(mine, k) for k in range(1, chips)]
        return both_cores(sum(g.astype(F32) for g in got).astype(BF16))

    def sum_scattered(part):
        mine = core_sum(part).astype(BF16)
        n = mine.shape[0] // chips
        mine = mine.reshape(chips, n, width)
        got = [pick(mine, chip)] + [to_chip(pick(mine, chip ^ k), k) for k in range(1, chips)]
        total = sum(g.astype(F32) for g in got).astype(BF16)
        have = jnp.stack([total] + [to_chip(total, k) for k in range(1, chips)])
        have = jnp.concatenate([pick(have, chip ^ k) for k in range(chips)])
        return both_cores(have)

    right = left = tiers
    early, late = [tiers], []
    for s in range(1, depth):
        right = lax.ppermute(right, "dp", [(j, j + 1) for j in range(s - 1, depth - 1)])
        left = lax.ppermute(left, "dp", [(j + 1, j) for j in range(depth - s)])
        if 2 * s < depth:
            early += [right, left]
        else:
            late.append(jnp.where(z >= s, right, left))
    slots = [sum_scattered(merge(jnp.concatenate(early)))]
    slots += [sum_direct(merge(x)) for x in late]
    v = jnp.concatenate(slots)
    offsets = [0]
    for s in range(1, depth):
        offsets += [-s, s] if 2 * s < depth else [0]
    n_slots = len(offsets)
    chunk_of = []
    s = 0
    for i, o in enumerate(offsets):
        if i < len(early):
            k = z + o
            chunk_of.append(jnp.where((k >= 0) & (k < depth), k, depth))
        else:
            s = depth - (n_slots - i)
            k = jnp.where(z >= s, z - s, jnp.where(z + s < depth, z + s, depth))
            chunk_of.append(k)

    def slot_of(k):
        d = jnp.abs(k - z)
        near = jnp.where(k == z, 0, 2 * d - jnp.where(k < z, 1, 0))
        return jnp.where(2 * d < depth, near, len(early) + d - (depth + 1) // 2)

    both = around(jnp.stack([labels, token_ids]))
    all_labels, all_tokens = both[:, 0].reshape(rows), both[:, 1].reshape(rows)
    at = jnp.arange(rows, dtype=I32)
    before = at[None, :] < at[:, None]
    rank = jnp.sum((before & (all_labels[None, :] == all_labels[:, None])).astype(I32), axis=1)
    domain = all_labels[:, None] == jnp.arange(DOMAINS, dtype=I32)[None, :]
    allowed = jnp.sum(jnp.where(domain, quotas[None, :], 0), axis=1)
    trained = rank < allowed
    place = jnp.sum((before & trained[None, :]).astype(I32), axis=1)
    place = jnp.where(trained, place, -1)
    chosen = place[:, None] == jnp.arange(cap, dtype=I32)[None, :]

    v32 = v.astype(F32)
    squares = jnp.sum(v32 * v32, axis=1).reshape(n_slots, chunk)
    squares = jnp.stack([pick(squares, slot_of(k)) for k in range(depth)]).reshape(rows)
    squares = jnp.sum(around(squares), axis=0)
    scale = lax.rsqrt(squares / (width * depth) + EPS)

    own = rows // (groups * across)
    per_chunk = chunk // own
    k_own = member // per_chunk
    row0 = slot_of(k_own) * chunk + (member % per_chunk) * own
    v_own = lax.dynamic_slice(v, (row0, 0), (own, width)).astype(F32)
    s_own = lax.dynamic_slice(scale, (member * own,), (own,))
    normed = (v_own * s_own[:, None] * norm_gain[None, :]).astype(BF16)

    u = (v32 * norm_gain[None, :]).astype(BF16)
    sel = jnp.concatenate([chosen.astype(BF16).reshape(depth, chunk, cap), jnp.zeros((1, chunk, cap), BF16)])
    sel = jnp.concatenate([pick(sel, k) for k in chunk_of])
    compact = lax.dot_general(sel, u, (((0,), (0,)), ((), ())), preferred_element_type=F32).astype(BF16)
    starts = [min(o * owned, vocab - owned) for o in range(depth)]
    part = lax.dot_general(w_head, compact, (((0,), (1,)), ((), ())), preferred_element_type=F32).astype(BF16)
    part = jnp.stack([part[a : a + owned] for a in starts])
    to_left = to_right = jnp.zeros((owned, cap), BF16)
    for s in range(1, depth):
        a = pick(part, jnp.clip(z + s - depth, 0, depth - 1)).astype(F32) + to_left.astype(F32)
        b = pick(part, jnp.clip(z - s + depth, 0, depth - 1)).astype(F32) + to_right.astype(F32)
        to_left = lax.ppermute(a.astype(BF16), "dp", [(j, j - 1) for j in range(depth - s, depth)])
        to_right = lax.ppermute(b.astype(BF16), "dp", [(j, j + 1) for j in range(s)])
    logits = pick(part, z).astype(F32) + to_left.astype(F32) + to_right.astype(F32)

    def compacted(value):
        return jnp.sum(jnp.where(chosen, value[:, None], jnp.zeros((), value.dtype)), axis=0)

    logits = logits * compacted(scale)[None, :]
    begin = jnp.minimum(z * owned, vocab - owned)
    index = begin + jnp.arange(owned, dtype=I32)
    fresh = (index >= z * owned)[:, None]
    index = (member * vocab + index)[:, None]
    hit = fresh & (index == compacted(all_tokens)[None, :])
    sumexp = jnp.sum(jnp.where(fresh, jnp.exp(logits), 0.0), axis=0)
    target = jnp.sum(jnp.where(hit, logits, 0.0), axis=0)
    mine = jnp.concatenate([sumexp, target])
    n_all = groups * depth * across
    every = lax.all_to_all(jnp.broadcast_to(mine[None], (n_all, 2 * cap)), ("grp", "dp", "tp"), 0, 0, tiled=True)
    total = jnp.sum(every, axis=0)
    loss = jnp.log(total[:cap]) - total[cap:]
    chosen_own = lax.dynamic_slice(chosen, (z * chunk, 0), (chunk, cap))
    row_loss = jnp.sum(jnp.where(chosen_own, loss[None, :], 0.0), axis=1)
    return (normed, row_loss)


def solution(mesh):
    in_specs = (
        P("dp", PLANE),
        P(PLANE, "dp"),
        P("dp"),
        P("dp", PLANE),
        P("dp"),
        P("dp"),
        P(),
    )
    out_specs = (P(PLANE, "dp"), P("dp"))
    sizes = (mesh.shape["grp"], mesh.shape["dp"], mesh.shape["tp"])

    def body(*args):
        return on_device(sizes, *args)

    return jax.shard_map(body, mesh=mesh, in_specs=in_specs, out_specs=out_specs, check_vma=False)
```
